128 devices in a mesh: tm: 16 (over z_lo, y, core), band: 8 (over x, z_hi).
Axes of the slice: x: 4, y: 4, z: 4 (z_hi: 2, z_lo: 2; z = z_hi * 2 + z_lo), core: 2. Of those that a mesh axis runs over, the one named last changes fastest.
Arguments:
- voltages: bfloat16 [8, 2, 1024, 32768], P('band', None, None, 'tm'), may hold values from -6 to 6
- antenna_flags: int32 [8, 128, 1024], P('band', 'tm'), may hold values from 0 to 1, as said below
- channel_flags: int32 [8, 128], P('band', 'tm'), may hold values from 0 to 1, as said below
Outputs:
- running_vis: float32 [8, 16, 1024, 1024], P('band', 'tm')
- dump_vis: float32 [8, 1024, 1024], P('band', 'tm')
- kurtosis: float32 [8, 1024], P('band', 'tm')
The draws below stay inside these ranges and needn't reach their ends.
Inputs may be any that keep to these rules, and one draw needn't show every extreme that they name: `antenna_flags`: in the first flag interval of every segment of 8 intervals no signal input is dropped. `channel_flags`: every channel is kept in the first flag interval of at least one segment.
All inputs are finite; a program needn't handle non-finite values.
Results may differ from the reference program's by a relative error of at most 0.0003.
Values sent between devices are 32-bit elements; how exact they have to be, the bound alone decides.
No kernel may reach another device: no remote copies, remote signals or barrier semaphores. Data moves between devices by JAX's collectives and lax.ppermute only.
A program may use at most 192 MiB of HBM per device.

```python
import jax
import jax.numpy as jnp
from jax import lax

S = 1024
TS = 2048
SEGLEN = 256
SEG_DEV = 8
NB = 8
NSEG = 128
TSAMP = 32768
N_TM = 16
N_BAND = 8


def draw_antenna_flags(key, part):
    drawn = jax.random.randint(key, (NB, NSEG, S), 0, 8)
    interval = jnp.arange(NSEG, dtype=jnp.int32)[None, :, None]
    forced = interval % SEG_DEV == 0
    return jnp.where(forced | (drawn > 0), 1, 0).astype(jnp.int32)


def draw_channel_flags(key, part):
    drawn = jax.random.randint(key, (NB, NSEG), 0, 4)
    chosen = jax.random.randint(jax.random.fold_in(key, 7), (NB, 1), 0, NSEG // SEG_DEV) * SEG_DEV
    interval = jnp.arange(NSEG, dtype=jnp.int32)[None, :]
    forced = interval == chosen
    return jnp.where(forced | (drawn > 0), 1, 0).astype(jnp.int32)


def shard_levels(key, dims, shards, least, largest):
    factor_of = 1.0
    for axis_at, parts in shards:
        draws = jax.random.uniform(jax.random.fold_in(jax.random.fold_in(key, 6), axis_at), (parts,), jnp.float32, least / len(shards), largest / len(shards))
        factor_of = factor_of * jnp.repeat(jnp.exp(draws), dims[axis_at] // parts).reshape((-1,) + (1,) * (len(dims) - 1 - axis_at))
    return factor_of


def scatter_about(own_key, shape, deviation, reach, pieces=(), kind=jnp.bfloat16):
    factor_of = shard_levels(own_key, shape, pieces, -0.22, 0.18) if pieces else 1.0
    values = jax.random.normal(own_key, shape, jnp.float32) * deviation * factor_of
    return jnp.minimum(jnp.maximum(values, -reach), reach).astype(kind)


def setup_inputs(seed: int = 0) -> dict:
    streams_of = jax.random.split(jax.random.key(seed), 4)
    voltages = scatter_about(streams_of[0], (NB, 2, S, TSAMP), 1.0, 6.0, ((0, 8), (3, 16)))
    antenna_flags = draw_antenna_flags(jax.random.fold_in(streams_of[3], 71), 0)
    channel_flags = draw_channel_flags(jax.random.fold_in(streams_of[3], 71), 0)
    return dict(voltages=voltages, antenna_flags=antenna_flags, channel_flags=channel_flags)


def band_terms(voltages, antenna_flags, channel_flags):
    keep_weight = (channel_flags[:, None] * antenna_flags).astype(jnp.float32)
    keep_weight = jnp.swapaxes(keep_weight, 0, 1)
    keep_weight = jnp.repeat(keep_weight, SEGLEN, axis=1)
    masked = voltages.astype(jnp.float32) * keep_weight[None]
    energy = masked[0] * masked[0] + masked[1] * masked[1]
    moment_one = jnp.sum(energy, axis=-1)
    moment_two = jnp.sum(energy * energy, axis=-1)
    valid_count = jnp.sum(keep_weight, axis=-1)
    kurtosis = (valid_count + 1.0) / (valid_count - 1.0) * (valid_count * moment_two / (moment_one * moment_one) - 1.0)
    row_ids = jnp.arange(S, dtype=jnp.int32)
    upper_half = row_ids[:, None] <= row_ids[None, :]

    def segment(integrated, segment_index):
        segment_data = lax.dynamic_slice_in_dim(masked, segment_index * TS, TS, 2)
        real_part = jnp.einsum('rst,rut->su', segment_data, segment_data, precision=lax.Precision.HIGHEST)
        cross_term = jnp.einsum('st,ut->su', segment_data[1], segment_data[0], precision=lax.Precision.HIGHEST)
        imag_part = cross_term - jnp.swapaxes(cross_term, 0, 1)
        gram_block = jnp.where(upper_half, real_part, imag_part) / TSAMP
        integrated = integrated + gram_block
        return integrated, integrated

    dump_total, running = lax.scan(segment, jnp.zeros((S, S), jnp.float32), jnp.arange(N_TM, dtype=jnp.int32))
    return running, dump_total, kurtosis


def reference(voltages, antenna_flags, channel_flags):
    running_all = []
    total_all = []
    kurt_all = []
    for band_index in range(N_BAND):
        running, dump_total, kurtosis = band_terms(voltages[band_index], antenna_flags[band_index], channel_flags[band_index])
        running_all.append(running)
        total_all.append(dump_total)
        kurt_all.append(kurtosis)
    return jnp.stack(running_all), jnp.stack(total_all), jnp.stack(kurt_all)
```

```python
import functools

import jax
import jax.numpy as jnp
from jax import lax
from jax.experimental import pallas as pl
from jax.experimental.pallas import tpu as pltpu
from jax.sharding import Mesh
from jax.sharding import PartitionSpec as P

TM = ("tm_0", "tm_1", "tm_2")
CHUNKS = 2
MIB = 1 << 20
VM = pl.BlockSpec(memory_space=pltpu.VMEM)
SM = pl.BlockSpec(memory_space=pltpu.SMEM)
HB = pl.BlockSpec(memory_space=pl.ANY)


def f32(*shape):
    return jax.ShapeDtypeStruct(shape, jnp.float32)


def call(kernel, operands, in_specs, out_shape, out_specs, name, us, vmem=24, **more):
    return pl.pallas_call(
        kernel,
        in_specs=in_specs,
        out_shape=out_shape,
        out_specs=out_specs,
        name=name,
        cost_estimate=pl.CostEstimate(flops=int(us * 4e6), bytes_accessed=int(us * 1e6), transcendentals=0),
        compiler_params=pltpu.CompilerParams(vmem_limit_bytes=vmem * MIB),
        **more,
    )(*operands)


def prep_kernel(chan_ref, volts_ref, flags_ref, xr_ref, xi_ref, mom_ref):
    intervals, signals = flags_ref.shape
    seg = volts_ref.shape[3] // intervals
    sub = lax.broadcasted_iota(jnp.int32, (intervals, signals), 0)
    chan = jnp.zeros((intervals, signals), jnp.int32)
    for n in range(intervals):
        chan = jnp.where(sub == n, chan_ref[0, n], chan)
    keep = (flags_ref[...] * chan).astype(jnp.float32)
    columns = jnp.transpose(keep)
    one = jnp.zeros((signals, 128), jnp.float32)
    two = jnp.zeros((signals, 128), jnp.float32)
    for n in range(intervals):
        k = columns[:, n : n + 1]
        for at in range(n * seg, (n + 1) * seg, 128):
            xr = volts_ref[0, 0, :, at : at + 128].astype(jnp.float32) * k
            xi = volts_ref[0, 1, :, at : at + 128].astype(jnp.float32) * k
            xr_ref[:, at : at + 128] = xr.astype(jnp.bfloat16)
            xi_ref[:, at : at + 128] = xi.astype(jnp.bfloat16)
            p = xr * xr + xi * xi
            one = one + p
            two = two + p * p
    m0 = jnp.sum(keep, axis=0, keepdims=True) * seg
    m1 = jnp.sum(jnp.transpose(one), axis=0, keepdims=True)
    m2 = jnp.sum(jnp.transpose(two), axis=0, keepdims=True)
    mom_ref[0] = jnp.concatenate([m0, m1, m2, jnp.zeros((5, signals), jnp.float32)], axis=0)


def gram_kernel(mine, chunk, moments, scale, h_ref, xr_ref, xi_ref, mom_ref, out_ref):
    rows = xr_ref.shape[2] // CHUNKS
    w = h_ref[0] if mine else 1 - h_ref[0]
    at = pl.ds(chunk * rows, rows)
    ar = [xr_ref[c, w, at, :] for c in range(8)]
    ai = [xi_ref[c, w, at, :] for c in range(8)]
    nr = [-a for a in ar]
    nt = (((1,), (1,)), ((), ()))
    r = lax.broadcasted_iota(jnp.int32, (rows, 256), 0)
    col = lax.broadcasted_iota(jnp.int32, (rows, 256), 1)
    for j in range(4):
        br = xr_ref[2 * j : 2 * j + 2].reshape(256, -1)
        bi = xi_ref[2 * j : 2 * j + 2].reshape(256, -1)
        split = 2 * j + 2
        lhs1 = jnp.concatenate(ar[:split] + ai[2 * j :], axis=0)
        lhs2 = jnp.concatenate(ai[:split] + nr[2 * j :], axis=0)
        o = lax.dot_general(lhs1, br, nt, preferred_element_type=jnp.float32)
        o = o + lax.dot_general(lhs2, bi, nt, preferred_element_type=jnp.float32)
        o = o * scale
        for c in range(8):
            re = o[c * rows : (c + 1) * rows] if c < split else None
            im = o[(c + 2) * rows : (c + 3) * rows] if c >= 2 * j else None
            if re is None:
                block = im
            elif im is None:
                block = re
            else:
                row = r + (128 * (c - 2 * j) + 64 * w + chunk * rows)
                block = jnp.where(row <= col, re, im)
            for rt in range(rows // 8):
                for half in range(2):
                    t = (c // 4) * rows + rt * 8 + 2 * j + half
                    out_ref[c % 4, t] = block[rt * 8 : rt * 8 + 8, half * 128 : half * 128 + 128]
    if moments:
        lane = lax.broadcasted_iota(jnp.int32, (8, 128), 1)
        for q in range(4):
            low, high = mom_ref[q], mom_ref[4 + q]
            first = jnp.where(lane < 64, low, pltpu.roll(high, 64, 1))
            second = jnp.where(lane < 64, pltpu.roll(low, 64, 1), high)
            out_ref[q, 2 * rows] = jnp.where(w == 0, first, second)


def add_kernel(y_ref, mine_ref, theirs_ref, *out_refs):
    y = y_ref[0]
    for d in range(4):
        q = (y + d) % 4
        out_refs[d][...] = mine_ref[q] + theirs_ref[q]


def sum_kernel(*refs):
    refs[4][...] = (refs[0][...] + refs[1][...]) + (refs[2][...] + refs[3][...])


def scan_kernel(rows, moments, yz_ref, *refs):
    w = refs[:4]
    tot_ref, other_ref = refs[4:6]
    e = refs[6:10]
    dump_ref = refs[10]
    y, z = yz_ref[0], yz_ref[1]
    tiles = 2 * rows
    base = jnp.where(z == 1, 1.0, 0.0)
    vals = [w[d][:tiles] for d in range(4)]
    start = other_ref[:tiles] * base
    for d in range(4):
        total = start
        for k in range(4):
            if k != d:
                total = total + vals[k] * jnp.where((y + k) % 4 < (y + d) % 4, 1.0, 0.0)
        e[d][...] = total
    for ct in range(8):
        for rt in range(rows // 8):
            t = z * rows + rt * 8 + ct
            dump_ref[rt * 8 : rt * 8 + 8, ct * 128 : ct * 128 + 128] = tot_ref[t] + other_ref[t]
    if moments:
        m = tot_ref[tiles] + other_ref[tiles]
        m = jnp.where(z == 0, m, pltpu.roll(m, 64, 1))
        m0, m1, m2 = m[0:1], m[1:2], m[2:3]
        kurt = (m0 + 1.0) / (m0 - 1.0) * (m0 * m2 / (m1 * m1) - 1.0)
        refs[11][...] = kurt[:, :64]


def own_kernel(chunk, rows, yh_ref, *refs):
    p, c = refs[:4], refs[4:8]
    mine_ref = refs[8]
    refs = refs[9 + (chunk > 0) :]
    run_ref, send_ref, buf, sem = refs
    y, h = yh_ref[0], yh_ref[1]
    tiles = 2 * rows
    take_mine = jnp.where(h == 0, 1.0, 0.0)
    take_chip = 1.0 - take_mine
    copies = []
    for d in range(4):
        q = (y + d) % 4
        for z in range(2):
            for rt in range(rows // 8):
                t = z * rows + rt * 8
                pre = p[d][t : t + 8]
                chip = c[d][t : t + 8]
                run = pre + (mine_ref[q, t : t + 8] * take_mine + chip * take_chip)
                send_ref[q, t : t + 8] = pre + chip * take_mine
                for ct in range(8):
                    buf[d, z, rt * 8 : rt * 8 + 8, ct * 128 : ct * 128 + 128] = run[ct]
            row = pl.multiple_of(((z * 4 + q) * 2 + h) * 64 + chunk * rows, rows)
            copy = pltpu.make_async_copy(buf.at[d, z], run_ref.at[pl.ds(row, rows)], sem.at[d, z])
            copy.start()
            copies.append(copy)
    for copy in copies:
        copy.wait()


def rest_kernel(chunk, rows, h_ref, recv_ref, theirs_ref, old_ref, run_ref, buf, sem):
    h = h_ref[0]
    take = jnp.where(h == 0, 1.0, 0.0)
    copies = []
    for q in range(4):
        for z in range(2):
            for rt in range(rows // 8):
                t = z * rows + rt * 8
                run = recv_ref[q, t : t + 8] + theirs_ref[q, t : t + 8] * take
                for ct in range(8):
                    buf[q, z, rt * 8 : rt * 8 + 8, ct * 128 : ct * 128 + 128] = run[ct]
            row = pl.multiple_of(((z * 4 + q) * 2 + 1 - h) * 64 + chunk * rows, rows)
            copy = pltpu.make_async_copy(buf.at[q, z], run_ref.at[pl.ds(row, rows)], sem.at[q, z])
            copy.start()
            copies.append(copy)
    for copy in copies:
        copy.wait()


def shift(x, d):
    return lax.ppermute(x, "tm_1", [(j, (j + d) % 4) for j in range(4)])


def swap(x, axis):
    return lax.ppermute(x, axis, [(0, 1), (1, 0)])


def per_device(voltages, antenna_flags, channel_flags):
    signals, samples = voltages.shape[2:]
    total_samples = samples * lax.axis_size(TM)
    z, y, h = (lax.axis_index(a).astype(jnp.int32) for a in TM)
    hv, yv = h.reshape(1), y.reshape(1)
    yz, yh = jnp.stack([y, z]), jnp.stack([y, h])
    rows = 64 // CHUNKS
    tiles = 2 * rows

    xr, xi, mom = pl.pallas_call(
        prep_kernel,
        grid=(signals // 128,),
        in_specs=[
            SM,
            pl.BlockSpec((1, 2, 128, samples), lambda i: (0, 0, i, 0)),
            pl.BlockSpec((antenna_flags.shape[1], 128), lambda i: (0, i)),
        ],
        out_specs=[
            pl.BlockSpec((128, samples), lambda i: (i, 0)),
            pl.BlockSpec((128, samples), lambda i: (i, 0)),
            pl.BlockSpec((1, 8, 128), lambda i: (i, 0, 0)),
        ],
        out_shape=[
            jax.ShapeDtypeStruct((signals, samples), jnp.bfloat16),
            jax.ShapeDtypeStruct((signals, samples), jnp.bfloat16),
            f32(8, 8, 128),
        ],
        name="prep",
        compiler_params=pltpu.CompilerParams(vmem_limit_bytes=16 * MIB),
    )(channel_flags, voltages, antenna_flags[0])
    xr = xr.reshape(8, 2, 64, samples)
    xi = xi.reshape(8, 2, 64, samples)

    def gram(mine, s):
        last = s == 0
        return call(
            functools.partial(gram_kernel, mine, s, last, 1.0 / total_samples),
            (hv, xr, xi, mom), [SM, VM, VM, VM], f32(4, tiles + last, 8, 128), VM, "gram", 12 / CHUNKS / 2, 40,
        )

    theirs, got, mine, chip, arrived, sums, other = ({} for _ in range(7))
    prefix, back, dumps, kurtosis = {}, {}, {}, None
    for s in range(CHUNKS):
        n = tiles + (s == 0)
        theirs[s] = gram(False, s)
        got[s] = swap(theirs[s], "tm_2")
        mine[s] = gram(True, s)
        chip[s] = call(add_kernel, (yv, mine[s], got[s]), [SM, VM, VM], [f32(n, 8, 128)] * 4, [VM] * 4, "add", 1)
    for s in range(CHUNKS):
        arrived[s] = [chip[s][0]] + [shift(chip[s][(4 - d) % 4], (4 - d) % 4) for d in (1, 3, 2)]
        arrived[s] = [arrived[s][0], arrived[s][1], arrived[s][3], arrived[s][2]]
        n = tiles + (s == 0)
        sums[s] = call(sum_kernel, arrived[s], [VM] * 4, f32(n, 8, 128), VM, "sum", 1)
        other[s] = swap(sums[s], "tm_0")
    for s in range(CHUNKS):
        outs = [f32(tiles, 8, 128)] * 4 + [f32(rows, 1024)]
        if s == 0:
            outs = outs + [f32(1, 64)]
        res = call(
            functools.partial(scan_kernel, rows, s == 0),
            (yz, *arrived[s], sums[s], other[s]), [SM] + [VM] * 6, outs, [VM] * len(outs), "scan", 1.5,
        )
        dumps[s] = res[4]
        if s == 0:
            kurtosis = res[5]
        e = res[:4]
        prefix[s] = [e[0]] + [shift(e[(4 - d) % 4], (4 - d) % 4) for d in (1, 3, 2)]
        prefix[s] = [prefix[s][0], prefix[s][1], prefix[s][3], prefix[s][2]]
    running = None
    scratch = [pltpu.VMEM((4, 2, rows, 1024), jnp.float32), pltpu.SemaphoreType.DMA((4, 2))]
    for s in range(CHUNKS):
        operands = (yh, *prefix[s], *chip[s], mine[s]) + (() if s == 0 else (running,))
        running, send = call(
            functools.partial(own_kernel, s, rows),
            operands, [SM] + [VM] * 9 + [HB] * (s > 0),
            [f32(signals, signals), f32(4, tiles, 8, 128)], [HB, VM], "own", 2, 32,
            scratch_shapes=scratch, input_output_aliases={10: 0} if s else {},
        )
        back[s] = swap(send, "tm_2")
    for s in range(CHUNKS):
        running = call(
            functools.partial(rest_kernel, s, rows),
            (hv, back[s], theirs[s], running), [SM, VM, VM, HB], f32(signals, signals), HB, "rest", 2, 32,
            scratch_shapes=scratch, input_output_aliases={3: 0},
        )
    dump = jnp.concatenate([dumps[s] for s in range(CHUNKS)], axis=0)
    return running[None, None], dump[None], kurtosis


def solution(mesh):
    finer = Mesh(
        mesh.devices.reshape(2, 4, 2, mesh.shape["band"]), ("tm_0", "tm_1", "tm_2", "band")
    )
    return jax.shard_map(
        per_device,
        mesh=finer,
        in_specs=(P("band", None, None, TM), P("band", TM, None), P("band", TM)),
        out_specs=(P("band", TM, None, None), P("band", TM, None), P("band", TM)),
        check_vma=False,
    )
```
